32 devices in a mesh: lat: 8 (over y, x, core), lev: 4 (over z).
Axes of the slice: x: 2, y: 2, z: 4, core: 2. Of those that a mesh axis runs over, the one named last changes fastest.
Arguments:
- fourier: bfloat16 [64, 2560, 128], P('lev', 'lat'), may hold values from -6 to 6
- quad_weights: float32 [2560], P('lat'), may hold values from 0.005 to 0.05
- legendre: bfloat16 [2560, 64, 1280], P('lat'), may hold values from -6 to 6
- owner_pair: int32 [64], replicated, may hold values from 0 to 63, each once
Outputs:
- spectra: float32 [64, 64, 1280], P('lat', 'lev')
- energy: float32 [], replicated
The draws below stay inside these ranges and needn't reach their ends.
Inputs may be any that keep to these rules, and one draw needn't show every extreme that they name: `owner_pair`: a permutation of 0 to 63.
All inputs are finite; a program needn't handle non-finite values.
Results may differ from the reference program's by a relative error of at most 0.00094.
Values may be sent and summed in bfloat16 or wider, within the bound.
A program may use at most 192 MiB of HBM per device.

```python
import math
import jax
import jax.numpy as jnp
from jax import lax

TRUNC = 1280
NLAT = 2560
M_WIN = 128
SPACING = 10
LEVELS = 32
CHANNELS = 64
NPAIR = 64
PAIRLEN = 1280


def draw_fourier(key, part):
    base = jax.random.fold_in(key, 11)
    rough_key, common_key = jax.random.split(base)
    common_normal = jnp.clip(jax.random.normal(common_key, (CHANNELS, 1, M_WIN), jnp.float32), -4.0, 4.0)
    rough = jnp.clip(jax.random.normal(rough_key, (CHANNELS, NLAT, M_WIN), jnp.float32), -4.0, 4.0)
    common = 0.3 * common_normal
    return (rough + common).astype(jnp.bfloat16)


def draw_legendre(key, part):
    base = jax.random.fold_in(key, 23)
    rough_key, mask_key, sign_key, pairing_key = jax.random.split(base, 4)
    pairing = jax.random.permutation(pairing_key, NPAIR).astype(jnp.int32)
    group = jnp.arange(NLAT, dtype=jnp.int32) * NPAIR // NLAT
    paired = group[:, None, None] == pairing[None, :, None]
    amplitude = jnp.where(paired, 3.0, 1.0)
    rough = jnp.clip(jax.random.normal(rough_key, (NLAT, NPAIR, PAIRLEN), jnp.float32), -4.0, 4.0)
    spike_size = 2.0
    diffuse = jnp.clip(amplitude * rough, -6.0, 6.0)
    chosen = jax.random.randint(mask_key, (NPAIR, PAIRLEN), 0, 64) == 0
    signs = (2 * jax.random.randint(sign_key, (NPAIR, PAIRLEN), 0, 2) - 1).astype(jnp.float32)
    spiked = signs[None, :, :] * spike_size + 0.25 * rough
    return jnp.where(chosen[None, :, :], spiked, diffuse).astype(jnp.bfloat16)


def steps_of(stream_key, dims, pieces, least, top_value):
    loudness = 1.0
    for position, blocks in pieces:
        draws = jax.random.uniform(jax.random.fold_in(jax.random.fold_in(stream_key, 6), position), (blocks,), jnp.float32, least / len(pieces), top_value / len(pieces))
        loudness = loudness * jnp.repeat(jnp.exp(draws), dims[position] // blocks).reshape((-1,) + (1,) * (len(dims) - 1 - position))
    return loudness


def setup_inputs(seed: int = 0) -> dict:
    streams_of = jax.random.split(jax.random.key(seed), 5)
    fourier = draw_fourier(jax.random.fold_in(streams_of[4], 71), 0)
    quad_weights = jnp.clip(jnp.exp(math.log(0.05) - 2.3025851 * jax.random.uniform(streams_of[1], (NLAT,), jnp.float32) ** steps_of(streams_of[1], (NLAT,), ((0, 8),), -0.2, 0.2)), 0.005, 0.05)
    legendre = draw_legendre(jax.random.fold_in(streams_of[4], 71), 0)
    owner_pair = jax.random.permutation(streams_of[3], NPAIR).astype(jnp.int32)
    return dict(fourier=fourier, quad_weights=quad_weights, legendre=legendre, owner_pair=owner_pair)


def reference(fourier, quad_weights, legendre, owner_pair):
    weighted = (fourier.astype(jnp.float32) * quad_weights[None, :, None]).astype(jnp.bfloat16)
    column_ids = jnp.arange(PAIRLEN, dtype=jnp.int32)

    def one_pair(pair_id):
        legendre_part = legendre[:, pair_id, :]
        low_wave = weighted[:, :, pair_id]
        high_wave = weighted[:, :, M_WIN - 1 - pair_id]
        low_part = jnp.dot(low_wave, legendre_part, preferred_element_type=jnp.float32)
        high_part = jnp.dot(high_wave, legendre_part, preferred_element_type=jnp.float32)
        low_limit = TRUNC - SPACING * pair_id - SPACING // 2
        return jnp.where(column_ids[None, :] < low_limit, low_part, high_part)

    spectra = lax.map(one_pair, owner_pair)
    channel_ids = jnp.arange(2 * LEVELS, dtype=jnp.int32)
    level_factor = 1.0 + 2.0 * (channel_ids // 2).astype(jnp.float32) / (LEVELS - 1)
    energy = jnp.sum(level_factor[None, :, None] * spectra * spectra) / (NPAIR * 2 * LEVELS * PAIRLEN)
    return (spectra, energy)
```

```python
import functools

import jax
import jax.numpy as jnp
from jax import lax
from jax.experimental import pallas as pl
from jax.experimental.pallas import tpu as pltpu
from jax.sharding import PartitionSpec as P

SPACING = 10
GROUP = 8
HALVES = 2
MESH = pl.DeviceIdType.MESH


def remote(src, dst, send, recv, device):
    return pltpu.make_async_remote_copy(
        src_ref=src, dst_ref=dst, send_sem=send, recv_sem=recv, device_id=device, device_id_type=MESH
    )


def kernel(
    cfg,
    owner_ref,
    wave_ref,
    leg_ref,
    out_ref,
    energy_ref,
    lhs,
    part,
    pair_out,
    pair_in,
    chip_out,
    chip_in,
    esum,
    elat,
    elev,
    pair_send,
    pair_recv,
    chip_send,
    chip_recv,
    elat_send,
    elat_recv,
    elev_send,
    elev_recv,
):
    n_lat, n_lev, ch, lats, pairs, length, width, steps, m_win = cfg
    t = pl.program_id(0)
    h = pl.program_id(1)
    lat = lax.axis_index("lat")
    lev = lax.axis_index("lev")
    core = lax.rem(lat, 2)
    chip = lat // 2
    chips = n_lat // 2
    own = pairs // n_lat
    rows = GROUP * ch
    groups = pairs // GROUP
    half_groups = groups // HALVES
    barrier = pltpu.get_barrier_semaphore()

    @pl.when((t == 0) & (h == 0))
    def _():
        for d in range(1, n_lat):
            pl.semaphore_signal(
                barrier, inc=1, device_id=(lax.rem(lat + d, n_lat), lev), device_id_type=MESH
            )
        for d in range(1, n_lev):
            pl.semaphore_signal(
                barrier, inc=1, device_id=(lat, lax.rem(lev + d, n_lev)), device_id_type=MESH
            )
        esum[...] = jnp.zeros_like(esum)

    @pl.when(t == 0)
    def _():
        def build(step, carry):
            g = h * half_groups + step
            for start in range(0, lats * GROUP, 256):
                size = min(256, lats * GROUP - start)
                first = start // GROUP
                base = first // 128 * 128
                depth = min(128, lats - base)
                src = lax.broadcasted_iota(jnp.int32, (depth, size), 0)
                dst = lax.broadcasted_iota(jnp.int32, (depth, size), 1)
                spread = (src == dst // GROUP + (first - base)).astype(jnp.float32).astype(jnp.bfloat16)
                row = lax.broadcasted_iota(jnp.int32, (rows, size), 0) // ch
                col = lax.rem(lax.broadcasted_iota(jnp.int32, (rows, size), 1), GROUP)
                for side in range(2):
                    j = g * GROUP if side == 0 else m_win - GROUP - g * GROUP
                    w = wave_ref[pl.ds(pl.multiple_of(j * ch, rows), rows), base : base + depth]
                    x = jnp.dot(w, spread, preferred_element_type=jnp.float32)
                    keep = row == (col if side == 0 else GROUP - 1 - col)
                    lhs[g, side * rows : (side + 1) * rows, start : start + size] = jnp.where(
                        keep, x, 0.0
                    ).astype(jnp.bfloat16)
            return carry

        lax.fori_loop(0, half_groups, build, 0)

    slot = lax.rem(t, 2)
    col_ids = t * width + lax.broadcasted_iota(jnp.int32, (ch, width), 1)

    for step in range(half_groups):
        g = h * half_groups + step
        rhs = leg_ref[:, step * GROUP : (step + 1) * GROUP, :].reshape(lats * GROUP, width)
        both = jnp.dot(lhs[g], rhs, preferred_element_type=jnp.float32)
        for i in range(GROUP):
            p = g * GROUP + i
            low = both[i * ch : (i + 1) * ch]
            high = both[rows + (GROUP - 1 - i) * ch : rows + (GROUP - i) * ch]
            limit = length - SPACING * p - SPACING // 2
            part[slot, p] = jnp.where(col_ids < limit, low, high)

    def pair_copy(u):
        return remote(
            pair_out.at[u], pair_in.at[u], pair_send.at[u], pair_recv.at[u],
            (2 * chip + 1 - core, lev),
        )

    def chip_copy(u, d):
        return remote(
            chip_out.at[u, d - 1], chip_in.at[u, d - 1],
            chip_send.at[u, d - 1], chip_recv.at[u, d - 1],
            (2 * lax.rem(chip + d, chips) + core, lev),
        )

    def to_partner(u):
        s = lax.rem(u, 2)
        for d in range(chips):
            q = lax.rem(chip + d, chips)
            for o in range(own):
                pair_id = owner_ref[(2 * q + 1 - core) * own + o]
                pair_out[u, d * own + o] = part[s, pair_id]
        pair_copy(u).start()

    def columns(u):
        return pl.ds(pl.multiple_of(u * width, width), width)

    def to_chips(u):
        s = lax.rem(u, 2)
        pair_copy(u).wait_recv()
        for d in list(range(1, chips)) + [0]:
            q = lax.rem(chip + d, chips)
            for o in range(own):
                pair_id = owner_ref[(2 * q + core) * own + o]
                total = part[s, pair_id] + pair_in[u, d * own + o]
                if d:
                    chip_out[u, d - 1, o] = total.astype(jnp.bfloat16)
                else:
                    out_ref[o, :, columns(u)] = total
            if d:
                chip_copy(u, d).start()

    channel = lev * ch + lax.broadcasted_iota(jnp.int32, (ch, width), 0)
    factor = 1.0 + 2.0 * (channel // 2).astype(jnp.float32) / (ch * n_lev // 2 - 1)

    def collect(u):
        for d in range(1, chips):
            chip_copy(u, d).wait_recv()
        acc = jnp.zeros((ch, width), jnp.float32)
        for o in range(own):
            total = out_ref[o, :, columns(u)]
            for d in range(1, chips):
                total = total + chip_in[u, d - 1, o].astype(jnp.float32)
            out_ref[o, :, columns(u)] = total
            acc = acc + total * total
        esum[...] += acc * factor

    @pl.when((t == 0) & (h == HALVES - 1))
    def _():
        pl.semaphore_wait(barrier, n_lat - 1 + n_lev - 1)

    @pl.when((h == 0) & (t >= 1))
    def _():
        to_chips(t - 1)

    @pl.when(h == HALVES - 1)
    def _():
        to_partner(t)

    @pl.when((h == HALVES - 1) & (t >= 2))
    def _():
        collect(t - 2)

    @pl.when((h == HALVES - 1) & (t == steps - 1))
    def _():
        if steps >= 2:
            collect(steps - 2)
        to_chips(steps - 1)
        collect(steps - 1)

        def exchange(buf, send, recv, me, n, device):
            def copy(idx, d):
                return remote(
                    buf.at[idx], buf.at[idx], send.at[d - 1], recv.at[idx],
                    device(lax.rem(me + d, n)),
                )

            for d in range(1, n):
                copy(me, d).start()
            for d in range(1, n):
                copy(lax.rem(me + n - d, n), d).wait_recv()
            for d in range(1, n):
                copy(me, d).wait_send()

        acc = esum[...]
        lanes = sum(acc[:, i : i + 128] for i in range(0, width, 128))
        elat[lat] = sum(lanes[i : i + 8] for i in range(0, ch, 8))
        exchange(elat, elat_send, elat_recv, lat, n_lat, lambda i: (i, lev))
        total = elat[0]
        for i in range(1, n_lat):
            total = total + elat[i]
        elev[lev] = total
        exchange(elev, elev_send, elev_recv, lev, n_lev, lambda i: (lat, i))
        total = elev[0]
        for i in range(1, n_lev):
            total = total + elev[i]
        energy_ref[...] = jnp.full((1, 1), jnp.sum(total)) / (pairs * ch * n_lev * length)

        for u in range(steps):
            pair_copy(u).wait_send()
            for d in range(1, chips):
                chip_copy(u, d).wait_send()


def shards(n_lat, n_lev, fourier, quad_weights, legendre, owner_pair):
    weighted = (fourier.astype(jnp.float32) * quad_weights[None, :, None]).astype(jnp.bfloat16)
    ch, lats, m_win = fourier.shape
    pairs, length = legendre.shape[1:]
    width = 256
    steps = length // width
    wave = jnp.transpose(weighted, (2, 0, 1)).reshape(m_win * ch, lats)
    own = pairs // n_lat
    chips = n_lat // 2
    cfg = (n_lat, n_lev, ch, lats, pairs, length, width, steps, m_win)
    dma = pltpu.SemaphoreType.DMA
    block = pairs // HALVES
    spectra, energy = pl.pallas_call(
        functools.partial(kernel, cfg),
        grid=(steps, HALVES),
        out_shape=(
            jax.ShapeDtypeStruct((own, ch, length), jnp.float32),
            jax.ShapeDtypeStruct((1, 1), jnp.float32),
        ),
        in_specs=[
            pl.BlockSpec(memory_space=pltpu.SMEM),
            pl.BlockSpec((m_win * ch, lats), lambda t, h: (0, 0)),
            pl.BlockSpec((lats, block, width), lambda t, h: (0, h, t)),
        ],
        out_specs=(
            pl.BlockSpec((own, ch, length), lambda t, h: (0, 0, 0)),
            pl.BlockSpec((1, 1), lambda t, h: (0, 0)),
        ),
        scratch_shapes=[
            pltpu.VMEM((pairs // GROUP, 2 * GROUP * ch, lats * GROUP), jnp.bfloat16),
            pltpu.VMEM((2, pairs, ch, width), jnp.float32),
            pltpu.VMEM((steps, pairs // 2, ch, width), jnp.float32),
            pltpu.VMEM((steps, pairs // 2, ch, width), jnp.float32),
            pltpu.VMEM((steps, chips - 1, own, ch, width), jnp.bfloat16),
            pltpu.VMEM((steps, chips - 1, own, ch, width), jnp.bfloat16),
            pltpu.VMEM((ch, width), jnp.float32),
            pltpu.VMEM((n_lat, 8, 128), jnp.float32),
            pltpu.VMEM((n_lev, 8, 128), jnp.float32),
            dma((steps,)),
            dma((steps,)),
            dma((steps, chips - 1)),
            dma((steps, chips - 1)),
            dma((n_lat - 1,)),
            dma((n_lat,)),
            dma((n_lev - 1,)),
            dma((n_lev,)),
        ],
        compiler_params=pltpu.CompilerParams(
            collective_id=0,
            has_side_effects=True,
            vmem_limit_bytes=60 * 1024 * 1024,
            dimension_semantics=("arbitrary", "arbitrary"),
        ),
    )(owner_pair, wave, legendre)
    return spectra, energy.reshape(())


def solution(mesh):
    return jax.shard_map(
        functools.partial(shards, mesh.shape["lat"], mesh.shape["lev"]),
        mesh=mesh,
        in_specs=(P("lev", "lat", None), P("lat"), P("lat", None, None), P()),
        out_specs=(P("lat", "lev", None), P()),
        check_vma=False,
    )
```

```python
import functools

import jax
import jax.numpy as jnp
from jax import lax
from jax.experimental import pallas as pl
from jax.experimental.pallas import tpu as pltpu
from jax.sharding import PartitionSpec as P

SPACING = 10
GROUP = 8
HALVES = 2
MESH = pl.DeviceIdType.MESH


def remote(src, dst, send, recv, device):
    return pltpu.make_async_remote_copy(
        src_ref=src, dst_ref=dst, send_sem=send, recv_sem=recv, device_id=device, device_id_type=MESH
    )


def kernel(
    cfg,
    owner_ref,
    wave_ref,
    leg_ref,
    out_ref,
    energy_ref,
    lhs,
    part,
    pair_out,
    pair_in,
    chip_out,
    chip_in,
    esum,
    elat,
    elev,
    pair_send,
    pair_recv,
    chip_send,
    chip_recv,
    elat_send,
    elat_recv,
    elev_send,
    elev_recv,
):
    n_lat, n_lev, ch, lats, pairs, length, width, steps, m_win = cfg
    t = pl.program_id(0)
    h = pl.program_id(1)
    lat = lax.axis_index("lat")
    lev = lax.axis_index("lev")
    core = lax.rem(lat, 2)
    chip = lat // 2
    chips = n_lat // 2
    own = pairs // n_lat
    rows = GROUP * ch
    groups = pairs // GROUP
    half_groups = groups // HALVES
    barrier = pltpu.get_barrier_semaphore()

    @pl.when((t == 0) & (h == 0))
    def _():
        for d in range(1, n_lat):
            pl.semaphore_signal(
                barrier, inc=1, device_id=(lax.rem(lat + d, n_lat), lev), device_id_type=MESH
            )
        for d in range(1, n_lev):
            pl.semaphore_signal(
                barrier, inc=1, device_id=(lat, lax.rem(lev + d, n_lev)), device_id_type=MESH
            )
        esum[...] = jnp.zeros_like(esum)

    late = int(steps > 1 and width <= length - SPACING * (pairs - 1) - SPACING // 2)

    def build_side(side):
        def build(step, carry):
            g = h * half_groups + step
            for start in range(0, lats * GROUP, 256):
                size = min(256, lats * GROUP - start)
                first = start // GROUP
                base = first // 128 * 128
                depth = min(128, lats - base)
                src = lax.broadcasted_iota(jnp.int32, (depth, size), 0)
                dst = lax.broadcasted_iota(jnp.int32, (depth, size), 1)
                spread = (src == dst // GROUP + (first - base)).astype(jnp.float32).astype(jnp.bfloat16)
                row = lax.broadcasted_iota(jnp.int32, (rows, size), 0) // ch
                col = lax.rem(lax.broadcasted_iota(jnp.int32, (rows, size), 1), GROUP)
                j = g * GROUP if side == 0 else m_win - GROUP - g * GROUP
                w = wave_ref[pl.ds(pl.multiple_of(j * ch, rows), rows), base : base + depth]
                x = jnp.dot(w, spread, preferred_element_type=jnp.float32)
                keep = row == (col if side == 0 else GROUP - 1 - col)
                lhs[g, side * rows : (side + 1) * rows, start : start + size] = jnp.where(
                    keep, x, 0.0
                ).astype(jnp.bfloat16)
            return carry

        lax.fori_loop(0, half_groups, build, 0)

    @pl.when(t == 0)
    def _():
        build_side(0)

    @pl.when(t == late)
    def _():
        build_side(1)

    slot = lax.rem(t, 2)
    col_ids = t * width + lax.broadcasted_iota(jnp.int32, (ch, width), 1)

    for step in range(half_groups):
        g = h * half_groups + step
        span = slice(step * GROUP, (step + 1) * GROUP)
        top = length - SPACING * GROUP * g - SPACING // 2
        is_low = (t + 1) * width <= top - SPACING * (GROUP - 1)
        is_high = t * width >= top

        @pl.when(is_low | is_high)
        def _():
            side = is_high.astype(jnp.int32)
            rhs = leg_ref[:, span, :].reshape(lats * GROUP, width)
            left = lhs[g, pl.ds(pl.multiple_of(side * rows, rows), rows), :]
            one = jnp.dot(left, rhs, preferred_element_type=jnp.float32)
            for i in range(GROUP):
                p = g * GROUP + i + side * (GROUP - 1 - 2 * i)
                part[slot, p] = one[i * ch : (i + 1) * ch]

        @pl.when(jnp.logical_not(is_low | is_high))
        def _():
            rhs = leg_ref[:, span, :].reshape(lats * GROUP, width)
            both = jnp.dot(lhs[g], rhs, preferred_element_type=jnp.float32)
            for i in range(GROUP):
                p = g * GROUP + i
                low = both[i * ch : (i + 1) * ch]
                high = both[rows + (GROUP - 1 - i) * ch : rows + (GROUP - i) * ch]
                limit = length - SPACING * p - SPACING // 2
                part[slot, p] = jnp.where(col_ids < limit, low, high)

    def pair_copy(u):
        return remote(
            pair_out.at[u], pair_in.at[u], pair_send.at[u], pair_recv.at[u],
            (2 * chip + 1 - core, lev),
        )

    def chip_copy(u, d):
        return remote(
            chip_out.at[u, d - 1], chip_in.at[u, d - 1],
            chip_send.at[u, d - 1], chip_recv.at[u, d - 1],
            (2 * lax.rem(chip + d, chips) + core, lev),
        )

    def to_partner(u):
        s = lax.rem(u, 2)
        for d in range(chips):
            q = lax.rem(chip + d, chips)
            for o in range(own):
                pair_id = owner_ref[(2 * q + 1 - core) * own + o]
                pair_out[u, d * own + o] = part[s, pair_id]
        pair_copy(u).start()

    def columns(u):
        return pl.ds(pl.multiple_of(u * width, width), width)

    def to_chips(u):
        s = lax.rem(u, 2)
        pair_copy(u).wait_recv()
        for d in list(range(1, chips)) + [0]:
            q = lax.rem(chip + d, chips)
            for o in range(own):
                pair_id = owner_ref[(2 * q + core) * own + o]
                total = part[s, pair_id] + pair_in[u, d * own + o]
                if d:
                    chip_out[u, d - 1, o] = total.astype(jnp.bfloat16)
                else:
                    out_ref[o, :, columns(u)] = total
            if d:
                chip_copy(u, d).start()

    channel = lev * ch + lax.broadcasted_iota(jnp.int32, (ch, width), 0)
    factor = 1.0 + 2.0 * (channel // 2).astype(jnp.float32) / (ch * n_lev // 2 - 1)

    def collect(u):
        for d in range(1, chips):
            chip_copy(u, d).wait_recv()
        acc = jnp.zeros((ch, width), jnp.float32)
        for o in range(own):
            total = out_ref[o, :, columns(u)]
            for d in range(1, chips):
                total = total + chip_in[u, d - 1, o].astype(jnp.float32)
            out_ref[o, :, columns(u)] = total
            acc = acc + total * total
        esum[...] += acc * factor

    @pl.when((t == 0) & (h == HALVES - 1))
    def _():
        pl.semaphore_wait(barrier, n_lat - 1 + n_lev - 1)

    @pl.when((h == 0) & (t >= 1))
    def _():
        to_chips(t - 1)

    @pl.when(h == HALVES - 1)
    def _():
        to_partner(t)

    @pl.when((h == HALVES - 1) & (t >= 2))
    def _():
        collect(t - 2)

    @pl.when((h == HALVES - 1) & (t == steps - 1))
    def _():
        if steps >= 2:
            collect(steps - 2)
        to_chips(steps - 1)
        collect(steps - 1)

        def exchange(buf, send, recv, me, n, device):
            def copy(idx, d):
                return remote(
                    buf.at[idx], buf.at[idx], send.at[d - 1], recv.at[idx],
                    device(lax.rem(me + d, n)),
                )

            for d in range(1, n):
                copy(me, d).start()
            for d in range(1, n):
                copy(lax.rem(me + n - d, n), d).wait_recv()
            for d in range(1, n):
                copy(me, d).wait_send()

        acc = esum[...]
        lanes = sum(acc[:, i : i + 128] for i in range(0, width, 128))
        elat[lat] = sum(lanes[i : i + 8] for i in range(0, ch, 8))
        exchange(elat, elat_send, elat_recv, lat, n_lat, lambda i: (i, lev))
        total = elat[0]
        for i in range(1, n_lat):
            total = total + elat[i]
        elev[lev] = total
        exchange(elev, elev_send, elev_recv, lev, n_lev, lambda i: (lat, i))
        total = elev[0]
        for i in range(1, n_lev):
            total = total + elev[i]
        energy_ref[...] = jnp.full((1, 1), jnp.sum(total)) / (pairs * ch * n_lev * length)

        for u in range(steps):
            pair_copy(u).wait_send()
            for d in range(1, chips):
                chip_copy(u, d).wait_send()


def shards(n_lat, n_lev, fourier, quad_weights, legendre, owner_pair):
    weighted = (fourier.astype(jnp.float32) * quad_weights[None, :, None]).astype(jnp.bfloat16)
    ch, lats, m_win = fourier.shape
    pairs, length = legendre.shape[1:]
    width = 256
    steps = length // width
    wave = jnp.transpose(weighted, (2, 0, 1)).reshape(m_win * ch, lats)
    own = pairs // n_lat
    chips = n_lat // 2
    cfg = (n_lat, n_lev, ch, lats, pairs, length, width, steps, m_win)
    dma = pltpu.SemaphoreType.DMA
    block = pairs // HALVES
    spectra, energy = pl.pallas_call(
        functools.partial(kernel, cfg),
        grid=(steps, HALVES),
        out_shape=(
            jax.ShapeDtypeStruct((own, ch, length), jnp.float32),
            jax.ShapeDtypeStruct((1, 1), jnp.float32),
        ),
        in_specs=[
            pl.BlockSpec(memory_space=pltpu.SMEM),
            pl.BlockSpec((m_win * ch, lats), lambda t, h: (0, 0)),
            pl.BlockSpec((lats, block, width), lambda t, h: (0, h, t)),
        ],
        out_specs=(
            pl.BlockSpec((own, ch, length), lambda t, h: (0, 0, 0)),
            pl.BlockSpec((1, 1), lambda t, h: (0, 0)),
        ),
        scratch_shapes=[
            pltpu.VMEM((pairs // GROUP, 2 * GROUP * ch, lats * GROUP), jnp.bfloat16),
            pltpu.VMEM((2, pairs, ch, width), jnp.float32),
            pltpu.VMEM((steps, pairs // 2, ch, width), jnp.float32),
            pltpu.VMEM((steps, pairs // 2, ch, width), jnp.float32),
            pltpu.VMEM((steps, chips - 1, own, ch, width), jnp.bfloat16),
            pltpu.VMEM((steps, chips - 1, own, ch, width), jnp.bfloat16),
            pltpu.VMEM((ch, width), jnp.float32),
            pltpu.VMEM((n_lat, 8, 128), jnp.float32),
            pltpu.VMEM((n_lev, 8, 128), jnp.float32),
            dma((steps,)),
            dma((steps,)),
            dma((steps, chips - 1)),
            dma((steps, chips - 1)),
            dma((n_lat - 1,)),
            dma((n_lat,)),
            dma((n_lev - 1,)),
            dma((n_lev,)),
        ],
        compiler_params=pltpu.CompilerParams(
            collective_id=0,
            has_side_effects=True,
            vmem_limit_bytes=60 * 1024 * 1024,
            dimension_semantics=("arbitrary", "arbitrary"),
        ),
    )(owner_pair, wave, legendre)
    return spectra, energy.reshape(())


def solution(mesh):
    return jax.shard_map(
        functools.partial(shards, mesh.shape["lat"], mesh.shape["lev"]),
        mesh=mesh,
        in_specs=(P("lev", "lat", None), P("lat"), P("lat", None, None), P()),
        out_specs=(P("lat", "lev", None), P()),
        check_vma=False,
    )
```
